32 devices in a mesh: island: 2 (over x), own: 16 (over z, y, core).
Axes of the slice: x: 2, y: 2, z: 4, core: 2. Of those that a mesh axis runs over, the one named last changes fastest.
Arguments:
- master: float32 [8, 2048, 8192], P(None, ('island', 'own')), may hold values from -6 to 6
- momentum: float32 [8, 2048, 8192], P(None, ('island', 'own')), may hold values from -6 to 6
- deltas: float32 [2, 2048, 8192], P('island', None, 'own'), may hold values from -6 to 6
- old_path: int32 [2], replicated, may hold values from 0 to 255
- new_path: int32 [2], replicated, may hold values from 0 to 255
- path_module: int32 [256], replicated, may hold values from 0 to 7
- island_steps: int32 [2], replicated, may hold values from 1 to 9
Outputs:
- new_master: float32 [8, 2048, 8192], P(None, ('island', 'own'))
- new_momentum: float32 [8, 2048, 8192], P(None, ('island', 'own'))
- new_module: float32 [2, 2048, 8192], P('island', None, 'own')
The draws below stay inside these ranges and needn't reach their ends.
All inputs are finite; a program needn't handle non-finite values.
Results may differ from the reference program's by a relative error of at most 0.00007.
Values sent between devices are 32-bit elements; how exact they have to be, the bound alone decides.
A program may use at most 192 MiB of HBM per device.

```python
import jax
import jax.numpy as jnp
from jax import lax

R = 2048
C = 8192
MODULES = 8
PATHS = 256
ISL = 2


def place_ends(result, rng, smallest, high):
    place = [jax.random.randint(jax.random.fold_in(rng, axis), (), 0, length) for axis, length in enumerate(result.shape)]
    widest = result.shape.index(max(result.shape))
    beside = place[:widest] + [(place[widest] + 1) % result.shape[widest]] + place[widest + 1:]
    return result.at[tuple(place)].set(smallest).at[tuple(beside)].set(high)


def block_scale(key, extent, pieces, smallest, largest):
    factor_of, own = 1.0, jax.random.fold_in(key, 6)
    for axis_at, shards_of in pieces:
        heights = jnp.exp(jax.random.uniform(jax.random.fold_in(own, axis_at), (shards_of,), jnp.float32, smallest / len(pieces), largest / len(pieces)))
        factor_of = factor_of * jnp.repeat(heights, extent[axis_at] // shards_of).reshape([-1 if axis == axis_at else 1 for axis in range(len(extent))])
    return factor_of


def bell_draw(stream_key, shape, width, bound, shards=(), kind=jnp.bfloat16):
    result = jax.random.normal(stream_key, shape, jnp.float32) * width
    if len(shards) > 0:
        result = block_scale(stream_key, shape, shards, -0.22, 0.18) * result
    return jnp.clip(result, min=-bound, max=bound).astype(kind)


def setup_inputs(seed: int = 0) -> dict:
    keys = jax.random.split(jax.random.key(seed), 8)
    master = bell_draw(keys[0], (MODULES, R, C), 1.0, 6.0, ((1, 32),), jnp.float32)
    momentum = bell_draw(keys[1], (MODULES, R, C), 1.0, 6.0, ((1, 32),), jnp.float32)
    deltas = bell_draw(keys[2], (ISL, R, C), 1.0, 6.0, ((0, 2), (2, 16)), jnp.float32)
    old_path = jax.random.randint(keys[3], (ISL,), 0, PATHS).astype(jnp.int32)
    new_path = jax.random.randint(keys[4], (ISL,), 0, PATHS).astype(jnp.int32)
    path_module = place_ends(jax.random.randint(keys[5], (PATHS,), 0, MODULES), jax.random.fold_in(keys[5], 1), 0, MODULES - 1).astype(jnp.int32)
    island_steps = jax.random.randint(keys[6], (ISL,), 1, 10).astype(jnp.int32)
    return {"master": master, "momentum": momentum, "deltas": deltas, "old_path": old_path, "new_path": new_path, "path_module": path_module, "island_steps": island_steps}


def reference(master, momentum, deltas, old_path, new_path, path_module, island_steps):
    old_module = path_module[old_path].astype(jnp.int32)
    chosen = old_module[None, :] == jnp.arange(MODULES, dtype=jnp.int32)[:, None]
    mixing = chosen.astype(jnp.float32) * island_steps.astype(jnp.float32)[None, :]
    divisor = jnp.maximum(jnp.sum(mixing, axis=1), 1.0)
    average = jnp.einsum("kj,jrc->krc", mixing, deltas, precision=lax.Precision.HIGHEST)
    average = average / divisor[:, None, None]
    new_momentum = 0.9 * momentum + average
    new_master = master - 0.7 * (average + 0.9 * new_momentum)
    new_index = path_module[new_path].astype(jnp.int32)
    new_module = jnp.take(new_master, new_index, axis=0)
    return new_master, new_momentum, new_module
```

```python
import functools

import jax
import jax.numpy as jnp
from jax import lax
from jax.experimental import pallas as pl
from jax.experimental.pallas import tpu as pltpu
from jax.sharding import PartitionSpec as P


def mix(weight_ref, k, received, isles):
    total = weight_ref[k, 0] * received[0]
    for j in range(1, isles):
        total = total + weight_ref[k, j] * received[j]
    return total


def step(master, momentum, average):
    new_momentum = 0.9 * momentum + average
    return master - 0.7 * (average + 0.9 * new_momentum), new_momentum


def pick_kernel(isles, per, width, index_ref, weight_ref, master_ref, momentum_ref, received_ref, out_ref):
    k = index_ref[pl.program_id(0)]
    for p in range(per):
        columns = slice(p * width, (p + 1) * width)
        average = mix(weight_ref, k, [received_ref[j, p] for j in range(isles)], isles)
        out_ref[0, p] = step(master_ref[0, :, columns], momentum_ref[0, :, columns], average)[0]


def update_kernel(isles, modules, per, width, weight_ref, master_ref, momentum_ref, received_ref, new_master_ref, new_momentum_ref):
    for p in range(per):
        columns = slice(p * width, (p + 1) * width)
        received = [received_ref[j, p] for j in range(isles)]
        for k in range(modules):
            average = mix(weight_ref, k, received, isles)
            new_master, new_momentum = step(master_ref[k, :, columns], momentum_ref[k, :, columns], average)
            new_master_ref[k, :, columns] = new_master
            new_momentum_ref[k, :, columns] = new_momentum


def divisor_below(count, bound):
    return max(d for d in range(1, count + 1) if count % d == 0 and d <= max(bound, 1))


def pick(master, momentum, received, index, weight):
    modules, rows, _ = master.shape
    isles, owners, _, width = received.shape
    per = divisor_below(owners, (1 << 20) // (rows * width * 4))
    return pl.pallas_call(
        functools.partial(pick_kernel, isles, per, width),
        grid_spec=pltpu.PrefetchScalarGridSpec(
            num_scalar_prefetch=2,
            grid=(isles, owners // per),
            in_specs=[
                pl.BlockSpec((1, rows, per * width), lambda j, c, index, weight: (index[j], 0, c)),
                pl.BlockSpec((1, rows, per * width), lambda j, c, index, weight: (index[j], 0, c)),
                pl.BlockSpec((isles, per, rows, width), lambda j, c, index, weight: (0, c, 0, 0)),
            ],
            out_specs=pl.BlockSpec((1, per, rows, width), lambda j, c, index, weight: (j, c, 0, 0)),
        ),
        out_shape=jax.ShapeDtypeStruct((isles, owners, rows, width), jnp.float32),
        compiler_params=pltpu.CompilerParams(vmem_limit_bytes=32 << 20),
        cost_estimate=pl.CostEstimate(flops=8 * received.size, bytes_accessed=4 * 5 * received.size, transcendentals=0),
        name="pick",
    )(index, weight, master, momentum, received)


def update(master, momentum, received, weight):
    modules, rows, columns = master.shape
    isles, owners, _, width = received.shape
    per = divisor_below(owners, (2 << 20) // (modules * rows * width * 4))
    big = pl.BlockSpec((modules, rows, per * width), lambda c, weight: (0, 0, c))
    return pl.pallas_call(
        functools.partial(update_kernel, isles, modules, per, width),
        grid_spec=pltpu.PrefetchScalarGridSpec(
            num_scalar_prefetch=1,
            grid=(owners // per,),
            in_specs=[big, big, pl.BlockSpec((isles, per, rows, width), lambda c, weight: (0, c, 0, 0))],
            out_specs=[big, big],
        ),
        out_shape=[jax.ShapeDtypeStruct(master.shape, jnp.float32)] * 2,
        compiler_params=pltpu.CompilerParams(vmem_limit_bytes=40 << 20),
        cost_estimate=pl.CostEstimate(flops=8 * master.size, bytes_accessed=4 * 4 * master.size + 4 * received.size, transcendentals=0),
        name="update",
    )(weight, master, momentum, received)


def shards(master, momentum, deltas, old_path, new_path, path_module, island_steps):
    modules, rows, _ = master.shape
    owners = lax.axis_size("own")
    isles = lax.axis_size("island")
    width = deltas.shape[2]
    old_module = path_module[old_path]
    chosen = old_module[None, :] == jnp.arange(modules, dtype=jnp.int32)[:, None]
    mixing = chosen.astype(jnp.float32) * island_steps.astype(jnp.float32)[None, :]
    divisor = jnp.maximum(jnp.sum(mixing, axis=1), 1.0)
    weight = mixing / divisor[:, None]
    index = path_module[new_path]

    blocks = deltas.reshape(isles * owners, rows, width)
    received = lax.all_to_all(blocks, ("island", "own"), split_axis=0, concat_axis=0, tiled=True)
    received = received.reshape(isles, owners, rows, width)
    picked = pick(master, momentum, received, index, weight)
    spread = lax.all_to_all(
        picked.reshape(isles * owners, rows, width), ("island", "own"), split_axis=0, concat_axis=0, tiled=True
    )
    new_master, new_momentum = update(master, momentum, received, weight)
    return (new_master, new_momentum, spread.reshape(deltas.shape))


def solution(mesh):
    return jax.shard_map(
        shards,
        mesh=mesh,
        in_specs=(
            P(None, ("island", "own"), None),
            P(None, ("island", "own"), None),
            P("island", None, "own"),
            P(),
            P(),
            P(),
            P(),
        ),
        out_specs=(
            P(None, ("island", "own"), None),
            P(None, ("island", "own"), None),
            P("island", None, "own"),
        ),
        check_vma=False,
    )
```
